32 devices in a mesh: fsdp: 8 (over z, y), cols: 4 (over x, core).
Axes of the slice: x: 2, y: 2, z: 4, core: 2. Of those that a mesh axis runs over, the one named last changes fastest.
Arguments:
- train_gate: bfloat16 [3584, 14336], P('fsdp', 'cols'), may hold values from -0.09375 to 0.09375
- low_gate: bfloat16 [3584, 16], P('fsdp'), may hold values from -0.09375 to 0.09375
- high_gate: bfloat16 [16, 14336], P(None, 'cols'), may hold values from -1.5 to 1.5
- train_up: bfloat16 [3584, 14336], P('fsdp', 'cols'), may hold values from -0.09375 to 0.09375
- low_up: bfloat16 [3584, 16], P('fsdp'), may hold values from -0.09375 to 0.09375
- high_up: bfloat16 [16, 14336], P(None, 'cols'), may hold values from -1.5 to 1.5
- train_down: bfloat16 [14336, 3584], P('cols', 'fsdp'), may hold values from -0.046875 to 0.046875
- low_down: bfloat16 [14336, 16], P('cols'), may hold values from -0.046875 to 0.046875
- high_down: bfloat16 [16, 3584], P(None, 'fsdp'), may hold values from -1.5 to 1.5
- norm_train: float32 [3584], P(('fsdp', 'cols')), may hold values from 0.25 to 1.75
- norm_step: float32 [3584], P(('fsdp', 'cols')), may hold values from -0.3 to 0.3
Outputs:
- serving_gate: bfloat16 [3584, 14336], P(None, 'cols')
- serving_up: bfloat16 [3584, 14336], P(None, 'cols')
- serving_down: bfloat16 [14336, 3584], P('cols')
- serve_norm: bfloat16 [3584], replicated
The draws below stay inside these ranges and needn't reach their ends.
All inputs are finite; a program needn't handle non-finite values.
Results may differ from the reference program's by a relative error of at most 0.001.
Values may be sent and summed in bfloat16 or wider, within the bound.
A program may use at most 256 MiB of HBM per device.

```python
import jax
import jax.numpy as jnp

D_MODEL = 3584
D_INNER = 14336
RANK = 16


def steps_of(stream_key, dims, shards, least, largest):
    factor_of = 1.0
    for position, shards_of in shards:
        heights = jax.random.uniform(jax.random.fold_in(jax.random.fold_in(stream_key, 6), position), (shards_of,), jnp.float32, least / len(shards), largest / len(shards))
        factor_of = factor_of * jnp.repeat(jnp.exp(heights), dims[position] // shards_of).reshape((-1,) + (1,) * (len(dims) - 1 - position))
    return factor_of


def gaussian(key, shape, width, reach, shards=(), dtype=jnp.bfloat16):
    entries = width * jax.random.normal(key, shape, jnp.float32)
    if shards:
        entries = entries * steps_of(key, shape, shards, -0.22, 0.18)
    return jnp.clip(entries, -reach, reach).astype(dtype)


def setup_inputs(seed: int = 0) -> dict:
    keys = jax.random.split(jax.random.key(seed), 12)
    return {
        "train_gate": gaussian(keys[0], (D_MODEL, D_INNER), D_MODEL ** -0.5, 0.09375, ((0, 8), (1, 4))),
        "low_gate": gaussian(keys[1], (D_MODEL, RANK), D_MODEL ** -0.5, 0.09375, ((0, 8),)),
        "high_gate": gaussian(keys[2], (RANK, D_INNER), RANK ** -0.5, 1.5, ((1, 4),)),
        "train_up": gaussian(keys[3], (D_MODEL, D_INNER), D_MODEL ** -0.5, 0.09375, ((0, 8), (1, 4))),
        "low_up": gaussian(keys[4], (D_MODEL, RANK), D_MODEL ** -0.5, 0.09375, ((0, 8),)),
        "high_up": gaussian(keys[5], (RANK, D_INNER), RANK ** -0.5, 1.5, ((1, 4),)),
        "train_down": gaussian(keys[6], (D_INNER, D_MODEL), D_INNER ** -0.5, 0.046875, ((0, 4), (1, 8))),
        "low_down": gaussian(keys[7], (D_INNER, RANK), D_INNER ** -0.5, 0.046875, ((0, 4),)),
        "high_down": gaussian(keys[8], (RANK, D_MODEL), RANK ** -0.5, 1.5, ((1, 8),)),
        "norm_train": jnp.clip(1.0 + 0.15 * jax.random.normal(keys[9], (D_MODEL,), jnp.float32), 0.25, 1.75),
        "norm_step": jnp.clip(jax.random.uniform(keys[10], (D_MODEL,), jnp.float32, -0.3, 0.3) * steps_of(keys[10], (D_MODEL,), ((0, 32),), -0.4, 0.0), -0.3, 0.3),
    }


mix_rate = 1.0


def reference(train_gate, low_gate, high_gate, train_up, low_up, high_up, train_down, low_down, high_down, norm_train, norm_step):
    whole_gate = train_gate.astype(jnp.float32) + mix_rate * jnp.dot(low_gate, high_gate, preferred_element_type=jnp.float32)
    whole_up = train_up.astype(jnp.float32) + mix_rate * jnp.dot(low_up, high_up, preferred_element_type=jnp.float32)
    whole_down = train_down.astype(jnp.float32) + mix_rate * jnp.dot(low_down, high_down, preferred_element_type=jnp.float32)
    serving_gate = whole_gate.astype(jnp.bfloat16)
    serving_up = whole_up.astype(jnp.bfloat16)
    serving_down = whole_down.astype(jnp.bfloat16)
    serve_norm = (norm_train + norm_step).astype(jnp.bfloat16)
    return serving_gate, serving_up, serving_down, serve_norm
```

```python
import functools

import jax
import jax.numpy as jnp
from jax import lax
from jax.experimental import pallas as pl
from jax.experimental.pallas import tpu as pltpu
from jax.sharding import PartitionSpec as P

MESH = pl.DeviceIdType.MESH
LANES = 128
SUBLANES = 16
mix_rate = 1.0


def merged(base, low, high):
    product = mix_rate * jnp.dot(low, high, preferred_element_type=jnp.float32)
    return (base.astype(jnp.float32) + product).astype(jnp.bfloat16)


def fold_of(width):
    fold = 1
    while width * fold % LANES:
        fold += 1
    return fold


def sends(k, depth, chunks):
    half = chunks // 2
    every, first, second = range(chunks), range(half), range(half, chunks)
    last = depth - 1
    down, up, side = [], [], [(k, 0, every)]
    if k > 0:
        down = [(z, 0, every) for z in range(k, depth)]
        if k == 1:
            down.append((k, 1, first))
        elif k == last:
            down.append((k, 1, every))
    if k < last:
        up = [(z, 0, every) for z in range(k, -1, -1)]
        if k == last - 1:
            up.append((k, 1, first))
        elif k == 0:
            up.append((k, 1, every))
    for z in sorted(set(range(depth)) - {k}, key=lambda z: abs(z - k)):
        if (k == 0 and z == 1) or (k == last and z == last - 1):
            side.append((z, 0, second))
        elif not (0 < k < last and ((k == 1 and z == 0) or (k == last - 1 and z == last))):
            side.append((z, 0, every))
    return [[(z, row, c) for z, row, cs in runs for c in cs] for runs in (down, up, side)]


def receives(k, depth, chunks):
    down = sends(k + 1, depth, chunks)[0] if k < depth - 1 else []
    up = sends(k - 1, depth, chunks)[1] if k > 0 else []
    side = [(z, 1 - row, c) for z, row, c in sends(k, depth, chunks)[2]]
    return [down, up, side]


def plan(k, depth, chunks):
    outs, ins = sends(k, depth, chunks), receives(k, depth, chunks)
    arrives = {item: (slot, s) for s, items in enumerate(ins) for slot, item in enumerate(items)}
    order = []
    for s, items in enumerate(outs):
        key = 0
        for slot, item in enumerate(items):
            if item[:2] != (k, 0):
                key = max(key, arrives[item][0] + 1, slot - 2)
            order.append((key, slot, s, item))
    return outs, ins, arrives, sorted(order)


def gather_kernel(n_fsdp, n_cols, parts, *refs):
    own = refs[:3]
    norm_ref = refs[3]
    out = refs[4:7]
    norms = refs[7]
    send_sem, recv_sem, local_sem, col_send, col_recv, row_send, row_recv = refs[8:]
    depth, chunks = n_fsdp // 2, 3 * parts
    here, col = lax.axis_index("fsdp"), lax.axis_index("cols")
    place, side = lax.div(here, 2), lax.rem(here, 2)

    barrier = pltpu.get_barrier_semaphore()
    for step in range(1, n_fsdp):
        peer = lax.rem(here + step, n_fsdp)
        pl.semaphore_signal(barrier, inc=1, device_id={"fsdp": peer}, device_id_type=MESH)
    for step in range(1, n_cols):
        peer = lax.rem(col + step, n_cols)
        pl.semaphore_signal(barrier, inc=1, device_id={"cols": peer}, device_id_type=MESH)
    pl.semaphore_wait(barrier, n_fsdp - 1 + n_cols - 1)

    def view(ref, c):
        rows = ref.shape[-2] // parts
        return pl.ds(c % parts * rows, rows)

    def landing(item):
        z, row, c = item
        block = 2 * z + (side if row == 0 else 1 - side)
        ref = out[c // parts]
        return ref.at[block, view(ref, c)]

    def source(k, item):
        z, row, c = item
        if (z, row) == (k, 0):
            ref = own[c // parts]
            return ref.at[view(ref, c)]
        return landing(item)

    def body(k):
        outs, ins, arrives, order = plan(k, depth, chunks)
        targets = (2 * (k - 1) + side, 2 * (k + 1) + side, 2 * k + 1 - side)
        waited = set()

        def copy(s, slot, item):
            return pltpu.make_async_remote_copy(
                src_ref=source(k, item),
                dst_ref=landing(item),
                send_sem=send_sem.at[s, slot],
                recv_sem=recv_sem.at[s, slot],
                device_id={"fsdp": targets[s]},
                device_id_type=MESH,
            )

        def arrive(s, slot):
            if (s, slot) in waited:
                return
            waited.add((s, slot))
            block = landing(ins[s][slot])
            pltpu.make_async_remote_copy(
                src_ref=block,
                dst_ref=block,
                send_sem=send_sem.at[s, slot],
                recv_sem=recv_sem.at[s, slot],
                device_id={"fsdp": targets[2]},
                device_id_type=MESH,
            ).wait_recv()

        for _, slot, s, item in order:
            if item[:2] != (k, 0):
                at, stream = arrives[item]
                arrive(stream, at)
            copy(s, slot, item).start()
        for slot in range(max(len(items) for items in ins)):
            for s in range(3):
                if slot < len(ins[s]):
                    arrive(s, slot)
        for s in range(3):
            for slot, item in enumerate(outs[s]):
                copy(s, slot, item).wait_send()

    mine = pltpu.make_async_copy(norm_ref, norms.at[here, col], local_sem.at[3])
    mine.start()
    for step in range(1, n_cols):
        pltpu.make_async_remote_copy(
            src_ref=norm_ref,
            dst_ref=norms.at[here, col],
            send_sem=col_send.at[step],
            recv_sem=col_recv.at[step],
            device_id={"cols": lax.rem(col + step, n_cols)},
            device_id_type=MESH,
        ).start()
    mine.wait()
    for step in range(1, n_cols):
        pltpu.make_async_remote_copy(
            src_ref=norm_ref,
            dst_ref=norms.at[here, lax.rem(col + n_cols - step, n_cols)],
            send_sem=col_send.at[step],
            recv_sem=col_recv.at[step],
            device_id={"cols": lax.rem(col + step, n_cols)},
            device_id_type=MESH,
        ).wait()

    def row_copy(step, block):
        return pltpu.make_async_remote_copy(
            src_ref=norms.at[here],
            dst_ref=norms.at[block],
            send_sem=row_send.at[step],
            recv_sem=row_recv.at[step],
            device_id={"fsdp": lax.rem(here + step, n_fsdp)},
            device_id_type=MESH,
        )

    for step in range(1, n_fsdp):
        row_copy(step, here).start()

    local = [pltpu.make_async_copy(own[a], out[a].at[here], local_sem.at[a]) for a in range(3)]
    for c in local:
        c.start()
    for k in range(depth):
        pl.when(place == k)(functools.partial(body, k))
    for c in local:
        c.wait()
    for step in range(1, n_fsdp):
        row_copy(step, lax.rem(here + n_fsdp - step, n_fsdp)).wait()


def gather(n_fsdp, n_cols, pieces, norm):
    parts = 2 if n_fsdp <= 8 else 1
    slots = 3 * parts * n_fsdp // 2
    anywhere = pl.BlockSpec(memory_space=pl.ANY)
    dma = pltpu.SemaphoreType.DMA
    return pl.pallas_call(
        functools.partial(gather_kernel, n_fsdp, n_cols, parts),
        out_shape=[jax.ShapeDtypeStruct((n_fsdp,) + p.shape, p.dtype) for p in pieces]
        + [jax.ShapeDtypeStruct((n_fsdp, n_cols) + norm.shape, norm.dtype)],
        in_specs=[anywhere] * 4,
        out_specs=[anywhere] * 4,
        scratch_shapes=[
            dma((3, slots)),
            dma((3, slots)),
            dma((4,)),
            dma((n_cols,)),
            dma((n_cols,)),
            dma((n_fsdp,)),
            dma((n_fsdp,)),
        ],
        compiler_params=pltpu.CompilerParams(collective_id=0, has_side_effects=True),
    )(*pieces, norm)


def unfold_kernel(fold, in_ref, out_ref):
    width = in_ref.shape[-1] // fold
    for p in range(fold):
        out_ref[p] = jnp.concatenate(
            [in_ref[0, j, :, p * width : (p + 1) * width] for j in range(fold)], axis=1
        )


def unfold(blocks, fold):
    count, rows, width = blocks.shape
    tile = next(t for t in (448, 224, 112, 16) if rows % t == 0)
    out = pl.pallas_call(
        functools.partial(unfold_kernel, fold),
        grid=(count // fold, rows // tile),
        out_shape=jax.ShapeDtypeStruct((fold, rows, count // fold * width), blocks.dtype),
        in_specs=[pl.BlockSpec((1, fold, tile, width), lambda z, r: (z, 0, r, 0))],
        out_specs=pl.BlockSpec((fold, tile, width), lambda z, r: (0, r, z)),
    )(blocks.reshape(count // fold, fold, rows, width))
    return out.reshape(fold * rows, -1)


def per_device(
    n_fsdp,
    n_cols,
    train_gate,
    low_gate,
    high_gate,
    train_up,
    low_up,
    high_up,
    train_down,
    low_down,
    high_down,
    norm_train,
    norm_step,
):
    gate = merged(train_gate, low_gate, high_gate)
    up = merged(train_up, low_up, high_up)
    down = merged(train_down, low_down, high_down)
    rows, width = down.shape
    fold = fold_of(width)
    down = jnp.concatenate(jnp.split(down, fold, axis=0), axis=1)
    length = norm_train.shape[0]
    norm = jnp.pad(norm_train + norm_step, (0, -length % LANES))
    norm = jnp.broadcast_to(norm[None], (8, norm.shape[0]))
    gates, ups, downs, norms = gather(n_fsdp, n_cols, (gate, up, down), norm)
    serve_norm = norms[:, :, 0, :length].reshape(-1).astype(jnp.bfloat16)
    return (
        gates.reshape(-1, gates.shape[-1]),
        ups.reshape(-1, ups.shape[-1]),
        unfold(downs, fold),
        serve_norm,
    )


def solution(mesh):
    return jax.shard_map(
        functools.partial(per_device, mesh.shape["fsdp"], mesh.shape["cols"]),
        mesh=mesh,
        in_specs=(
            P("fsdp", "cols"),
            P("fsdp", None),
            P(None, "cols"),
            P("fsdp", "cols"),
            P("fsdp", None),
            P(None, "cols"),
            P("cols", "fsdp"),
            P("cols", None),
            P(None, "fsdp"),
            P(("fsdp", "cols")),
            P(("fsdp", "cols")),
        ),
        out_specs=(P(None, "cols"), P(None, "cols"), P("cols", None), P()),
        check_vma=False,
    )
```
